32 devices in a mesh: row: 8 (over z, y), col: 4 (over x, core).
Axes of the slice: x: 2, y: 2, z: 4, core: 2. Of those that a mesh axis runs over, the one named last changes fastest.
Arguments:
- eigvecs: float32 [32768, 512], P('row', 'col'), may hold values from -6 to 6
- reflectors: float32 [2, 32768, 512], P(None, 'row', 'col'), may hold values from -0.03125 to 0.03125
- factors: float32 [2, 512, 512], replicated, may hold values from -1 to 2, as said below
- slab: float32 [2048, 32768], P('col', 'row'), may hold values from -0.03125 to 0.03125
Outputs:
- vectors: float32 [32768, 512], P('row', 'col')
- product: float32 [2048, 512], P('col', 'row')
The draws below stay inside these ranges and needn't reach their ends.
Inputs may be any that keep to these rules, and one draw needn't show every extreme that they name: Each of the two 512 x 512 factors is upper triangular, with diagonal entries between 1 and 2.
All inputs are finite; a program needn't handle non-finite values.
Results may differ from the reference program's by a relative error of at most 0.000088.
Values sent between devices are 32-bit elements; how exact they have to be, the bound alone decides.
A program may use at most 128 MiB of HBM per device.

```python
import jax
import jax.numpy as jnp
from jax import lax

N = 32768
B = 512
K = 512
SLAB = 2048


def draw_factors(key, part):
    upper_key = jax.random.fold_in(key, 11)
    diag_key = jax.random.fold_in(key, 23)
    upper = jax.random.normal(upper_key, (2, B, B), jnp.float32) / jnp.sqrt(jnp.float32(B))
    diag = jax.random.uniform(diag_key, (2, B), jnp.float32, 1.0, 2.0)
    upper = jnp.clip(upper, -0.9, 0.9)
    rows = lax.broadcasted_iota(jnp.int32, (2, B, B), 1)
    cols = lax.broadcasted_iota(jnp.int32, (2, B, B), 2)
    strict = jnp.where(cols > rows, upper, jnp.float32(0.0))
    return jnp.where(cols == rows, diag[:, :, None], strict)


def level_of(own_key, shape, cuts, smallest, top_value):
    gain, own = 1.0, jax.random.fold_in(own_key, 6)
    for dim, blocks in cuts:
        draws = jnp.exp(jax.random.uniform(jax.random.fold_in(own, dim), (blocks,), jnp.float32, smallest / len(cuts), top_value / len(cuts)))
        gain = gain * jnp.repeat(draws, shape[dim] // blocks).reshape([-1 if axis == dim else 1 for axis in range(len(shape))])
    return gain


def scatter_about(rng, shape, width, reach, shards=(), dtype=jnp.bfloat16):
    array = jax.random.normal(rng, shape, jnp.float32) * width
    if len(shards) > 0:
        array = level_of(rng, shape, shards, -0.22, 0.18) * array
    return jnp.clip(array, min=-reach, max=reach).astype(dtype)


def setup_inputs(seed: int = 0) -> dict:
    key_of = jax.random.split(jax.random.key(seed), 5)
    eigvecs = scatter_about(key_of[0], (N, K), 1.0, 6.0, ((0, 8), (1, 4)), jnp.float32)
    reflectors = scatter_about(key_of[1], (2, N, B), N ** -0.5, 0.03125, ((1, 8), (2, 4)), jnp.float32)
    factors = draw_factors(jax.random.fold_in(key_of[4], 71), 0)
    slab = scatter_about(key_of[3], (SLAB, N), N ** -0.5, 0.03125, ((0, 4), (1, 8)), jnp.float32)
    return dict(eigvecs=eigvecs, reflectors=reflectors, factors=factors, slab=slab)


def matmul(left, right):
    return jnp.dot(left, right, precision=lax.Precision.HIGHEST, preferred_element_type=jnp.float32)


def reference(eigvecs, reflectors, factors, slab):
    first_y = reflectors[0]
    second_y = reflectors[1]
    second_w = matmul(second_y.T, eigvecs)
    inner = eigvecs - matmul(matmul(second_y, factors[1]), second_w)
    first_w = matmul(first_y.T, inner)
    vectors = inner - matmul(matmul(first_y, factors[0]), first_w)
    product = matmul(slab, vectors)
    return vectors, product
```

```python
import functools

import jax
import jax.numpy as jnp
from jax import lax
from jax.experimental import pallas as pl
from jax.experimental.pallas import tpu as pltpu
from jax.sharding import PartitionSpec as P

MESH = pl.DeviceIdType.MESH


def dot(left, right, dims=((1,), (0,))):
    return lax.dot_general(
        left, right, (dims, ((), ())), precision=lax.Precision.HIGH, preferred_element_type=jnp.float32
    )


def tdot(left, right):
    return dot(left, right, ((0,), (0,)))


def sum_gather_kernel(nrow, ncol, m_ref, out_ref, recv, rs_send, rs_recv, a_send, a_recv, x_send, x_recv, c_send, c_recv):
    r, c = lax.axis_index("row"), lax.axis_index("col")
    pairs = ncol // 2
    mate = c + 1 - 2 * lax.rem(c, 2)

    def row_at(d):
        return lax.rem(r + d + nrow, nrow)

    def col_at(s):
        return lax.rem(c + 2 * s + ncol, ncol)

    barrier = pltpu.get_barrier_semaphore()
    for d in range(1, nrow):
        pl.semaphore_signal(barrier, inc=1, device_id=(row_at(d), c), device_id_type=MESH)
    for s in range(1, pairs):
        pl.semaphore_signal(barrier, inc=1, device_id=(r, col_at(s)), device_id_type=MESH)
    pl.semaphore_signal(barrier, inc=1, device_id=(r, mate), device_id_type=MESH)
    pl.semaphore_wait(barrier, nrow - 1 + pairs - 1 + 1)

    def scatter(d):
        return pltpu.make_async_remote_copy(
            m_ref.at[row_at(d)], recv.at[d], rs_send.at[d], rs_recv.at[d],
            device_id=(row_at(d), c), device_id_type=MESH)

    for d in range(1, nrow):
        scatter(d).start()
    total = m_ref[r]
    for d in range(1, nrow):
        scatter(d).wait_recv()
        total = total + recv[d]
    out_ref[c, r] = total

    def along_row(d):
        return pltpu.make_async_remote_copy(
            out_ref.at[c, r], out_ref.at[c, r], a_send.at[d], a_recv.at[d],
            device_id=(row_at(d), c), device_id_type=MESH)

    def across(s, d):
        chunk = out_ref.at[c, row_at(-d)]
        return pltpu.make_async_remote_copy(
            chunk, chunk, x_send.at[s, d], x_recv.at[s, d],
            device_id=(r, col_at(s)), device_id_type=MESH)

    def to_mate(s, d):
        chunk = out_ref.at[col_at(-s), row_at(-d)]
        return pltpu.make_async_remote_copy(
            chunk, chunk, c_send.at[s, d], c_recv.at[s, d],
            device_id=(r, mate), device_id_type=MESH)

    for s in range(1, pairs):
        across(s, 0).start()
    for d in range(1, nrow):
        along_row(d).start()
    to_mate(0, 0).start()
    for d in range(1, nrow):
        along_row(d).wait_recv()
        for s in range(1, pairs):
            across(s, d).start()
        to_mate(0, d).start()
    for d in range(nrow):
        for s in range(1, pairs):
            across(s, d).wait_recv()
            to_mate(s, d).start()
    for d in range(nrow):
        for s in range(pairs):
            to_mate(s, d).wait_recv()
    for d in range(1, nrow):
        scatter(d).wait_send()
        along_row(d).wait_send()
    for d in range(nrow):
        for s in range(pairs):
            to_mate(s, d).wait_send()
            if s:
                across(s, d).wait_send()


def sum_gather(m, nrow, ncol):
    chunk = (m.shape[0] // nrow, m.shape[1])
    pairs = ncol // 2
    sem = pltpu.SemaphoreType.DMA
    out = pl.pallas_call(
        functools.partial(sum_gather_kernel, nrow, ncol),
        out_shape=jax.ShapeDtypeStruct((ncol, nrow) + chunk, jnp.float32),
        in_specs=[pl.BlockSpec(memory_space=pltpu.VMEM)],
        out_specs=pl.BlockSpec(memory_space=pltpu.VMEM),
        scratch_shapes=[
            pltpu.VMEM((nrow,) + chunk, jnp.float32),
            sem((nrow,)), sem((nrow,)), sem((nrow,)), sem((nrow,)),
            sem((pairs, nrow)), sem((pairs, nrow)), sem((pairs, nrow)), sem((pairs, nrow)),
        ],
        compiler_params=pltpu.CompilerParams(collective_id=0, has_side_effects=True),
        cost_estimate=pl.CostEstimate(flops=0, bytes_accessed=60_000_000, transcendentals=0),
        name="sum_gather",
    )(m.reshape((nrow,) + chunk))
    return out.reshape((ncol,) + m.shape)


def sum_scatter_kernel(nrow, p_ref, out_ref, recv, send_sem, recv_sem):
    r = lax.axis_index("row")

    def row_at(d):
        return lax.rem(r + d, nrow)

    barrier = pltpu.get_barrier_semaphore()
    for d in range(1, nrow):
        pl.semaphore_signal(barrier, inc=1, device_id={"row": row_at(d)}, device_id_type=MESH)
    pl.semaphore_wait(barrier, nrow - 1)

    def scatter(d):
        return pltpu.make_async_remote_copy(
            p_ref.at[row_at(d)], recv.at[d], send_sem.at[d], recv_sem.at[d],
            device_id={"row": row_at(d)}, device_id_type=MESH)

    for d in range(1, nrow):
        scatter(d).start()
    total = p_ref[r]
    for d in range(1, nrow):
        scatter(d).wait_recv()
        total = total + recv[d]
    out_ref[...] = total
    for d in range(1, nrow):
        scatter(d).wait_send()


def sum_scatter(p, nrow):
    chunk = (p.shape[0] // nrow, p.shape[1])
    sem = pltpu.SemaphoreType.DMA
    return pl.pallas_call(
        functools.partial(sum_scatter_kernel, nrow),
        out_shape=jax.ShapeDtypeStruct(chunk, jnp.float32),
        in_specs=[pl.BlockSpec(memory_space=pltpu.VMEM)],
        out_specs=pl.BlockSpec(memory_space=pltpu.VMEM),
        scratch_shapes=[pltpu.VMEM((nrow,) + chunk, jnp.float32), sem((nrow,)), sem((nrow,))],
        compiler_params=pltpu.CompilerParams(collective_id=1, has_side_effects=True),
        cost_estimate=pl.CostEstimate(flops=0, bytes_accessed=30_000_000, transcendentals=0),
        name="sum_scatter",
    )(p.reshape((nrow,) + chunk))


def on_device(nrow, ncol, eigvecs, reflectors, factors, slab):
    c = lax.axis_index("col")
    even = lax.rem(c, 2) == 0
    pairs = ncol // 2
    own = eigvecs.shape[1]
    parts = pairs if pairs <= 2 else 1
    order = lax.rem(c // 2 - jnp.arange(pairs) + pairs, pairs) if parts > 1 else jnp.zeros((1,), jnp.int32)
    swap = [(i, i + 1 - 2 * (i % 2)) for i in range(ncol)]

    def cross(block):
        return [block] + [
            lax.ppermute(block, "col", [(i, (i + 2 * s) % ncol) for i in range(ncol)]) for s in range(1, pairs)
        ]

    def pair_up(blocks):
        mates = [lax.ppermute(block, "col", swap) for block in blocks]
        return [
            jnp.concatenate([jnp.where(even, a, b), jnp.where(even, b, a)], axis=1) for a, b in zip(blocks, mates)
        ]

    def gather(block):
        if pairs <= 2:
            return pair_up(cross(block))
        return [lax.all_gather(block, "col", axis=1, tiled=True)]

    def reorder(stacked):
        return jnp.take(stacked, order, axis=0).reshape((-1,) + stacked.shape[2:])

    second_y = gather(reflectors[1])
    first_y = gather(reflectors[0])
    all_x = gather(eigvecs)

    second_w = reorder(jnp.stack([tdot(y, eigvecs) for y in second_y]))
    right = jnp.concatenate([eigvecs, reflectors[1]], axis=1)
    mixed = reorder(jnp.stack([tdot(y, right) for y in first_y]))
    panel = second_w.shape[0]
    stacked = jnp.concatenate([second_w, mixed[:, :own], mixed[:, own:]])
    if pairs <= 2:
        sums = sum_gather(stacked, nrow, ncol)
    else:
        sums = lax.all_gather(lax.psum(stacked, "row"), "col")

    slab_second = [dot(y, slab, ((0,), (1,))) for y in second_y]
    slab_first = [dot(y, slab, ((0,), (1,))) for y in first_y]
    slab_x = reorder(jnp.stack([dot(x, slab, ((0,), (1,))) for x in all_x]))

    second_w, first_raw, gram = (
        jnp.transpose(sums[:, i * panel : (i + 1) * panel], (1, 0, 2)).reshape(panel, -1) for i in range(3)
    )
    second_tw = dot(factors[1], second_w)
    first_tw = dot(factors[0], first_raw - dot(gram, second_tw))

    def local(tw):
        return reorder(tw.reshape((parts, -1) + tw.shape[1:]))

    second_tw, first_tw = local(second_tw), local(first_tw)
    partial = slab_x - tdot(second_tw, jnp.concatenate(slab_second)) - tdot(first_tw, jnp.concatenate(slab_first))
    product = sum_scatter(partial, nrow)

    vectors = eigvecs
    width = panel // parts
    for blocks, tw in ((second_y, second_tw), (first_y, first_tw)):
        mine = lax.dynamic_slice_in_dim(tw, c * own, own, axis=1)
        for s, y in enumerate(blocks):
            vectors = vectors - dot(y, mine[s * width : (s + 1) * width])
    return vectors, product.T


def solution(mesh):
    return jax.shard_map(
        functools.partial(on_device, mesh.shape["row"], mesh.shape["col"]),
        mesh=mesh,
        in_specs=(P("row", "col"), P(None, "row", "col"), P(), P("col", "row")),
        out_specs=(P("row", "col"), P("col", "row")),
        check_vma=False,
    )
```

```python
import functools

import jax
import jax.numpy as jnp
from jax import lax
from jax.experimental import pallas as pl
from jax.experimental.pallas import tpu as pltpu
from jax.sharding import PartitionSpec as P

MESH = pl.DeviceIdType.MESH


def dot(left, right, dims=((1,), (0,))):
    return lax.dot_general(
        left, right, (dims, ((), ())), precision=lax.Precision.HIGH, preferred_element_type=jnp.float32
    )


def tdot(left, right):
    return dot(left, right, ((0,), (0,)))


def sum_gather_kernel(nrow, ncol, m_ref, out_ref, recv, rs_send, rs_recv, a_send, a_recv, x_send, x_recv, c_send, c_recv):
    r, c = lax.axis_index("row"), lax.axis_index("col")
    pairs = ncol // 2
    mate = c + 1 - 2 * lax.rem(c, 2)

    def row_at(d):
        return lax.rem(r + d + nrow, nrow)

    def col_at(s):
        return lax.rem(c + 2 * s + ncol, ncol)

    barrier = pltpu.get_barrier_semaphore()
    for d in range(1, nrow):
        pl.semaphore_signal(barrier, inc=1, device_id=(row_at(d), c), device_id_type=MESH)
    for s in range(1, pairs):
        pl.semaphore_signal(barrier, inc=1, device_id=(r, col_at(s)), device_id_type=MESH)
    pl.semaphore_signal(barrier, inc=1, device_id=(r, mate), device_id_type=MESH)
    pl.semaphore_wait(barrier, nrow - 1 + pairs - 1 + 1)

    def scatter(d):
        return pltpu.make_async_remote_copy(
            m_ref.at[row_at(d)], recv.at[d], rs_send.at[d], rs_recv.at[d],
            device_id=(row_at(d), c), device_id_type=MESH)

    for d in range(1, nrow):
        scatter(d).start()
    total = m_ref[r]
    for d in range(1, nrow):
        scatter(d).wait_recv()
        total = total + recv[d]
    out_ref[c, r] = total

    def along_row(d):
        return pltpu.make_async_remote_copy(
            out_ref.at[c, r], out_ref.at[c, r], a_send.at[d], a_recv.at[d],
            device_id=(row_at(d), c), device_id_type=MESH)

    def across(s, d):
        chunk = out_ref.at[c, row_at(-d)]
        return pltpu.make_async_remote_copy(
            chunk, chunk, x_send.at[s, d], x_recv.at[s, d],
            device_id=(r, col_at(s)), device_id_type=MESH)

    def to_mate(s, d):
        chunk = out_ref.at[col_at(-s), row_at(-d)]
        return pltpu.make_async_remote_copy(
            chunk, chunk, c_send.at[s, d], c_recv.at[s, d],
            device_id=(r, mate), device_id_type=MESH)

    for s in range(1, pairs):
        across(s, 0).start()
    for d in range(1, nrow):
        along_row(d).start()
    to_mate(0, 0).start()
    for d in range(1, nrow):
        along_row(d).wait_recv()
        for s in range(1, pairs):
            across(s, d).start()
        to_mate(0, d).start()
    for d in range(nrow):
        for s in range(1, pairs):
            across(s, d).wait_recv()
            to_mate(s, d).start()
    for d in range(nrow):
        for s in range(pairs):
            to_mate(s, d).wait_recv()
    for d in range(1, nrow):
        scatter(d).wait_send()
        along_row(d).wait_send()
    for d in range(nrow):
        for s in range(pairs):
            to_mate(s, d).wait_send()
            if s:
                across(s, d).wait_send()


def sum_gather(m, nrow, ncol):
    chunk = (m.shape[0] // nrow, m.shape[1])
    pairs = ncol // 2
    sem = pltpu.SemaphoreType.DMA
    out = pl.pallas_call(
        functools.partial(sum_gather_kernel, nrow, ncol),
        out_shape=jax.ShapeDtypeStruct((ncol, nrow) + chunk, jnp.float32),
        in_specs=[pl.BlockSpec(memory_space=pltpu.VMEM)],
        out_specs=pl.BlockSpec(memory_space=pltpu.VMEM),
        scratch_shapes=[
            pltpu.VMEM((nrow,) + chunk, jnp.float32),
            sem((nrow,)), sem((nrow,)), sem((nrow,)), sem((nrow,)),
            sem((pairs, nrow)), sem((pairs, nrow)), sem((pairs, nrow)), sem((pairs, nrow)),
        ],
        compiler_params=pltpu.CompilerParams(collective_id=0, has_side_effects=True),
        cost_estimate=pl.CostEstimate(flops=0, bytes_accessed=60_000_000, transcendentals=0),
        name="sum_gather",
    )(m.reshape((nrow,) + chunk))
    return out.reshape((ncol,) + m.shape)


def sum_scatter_kernel(nrow, p_ref, out_ref, recv, send_sem, recv_sem):
    r = lax.axis_index("row")

    def row_at(d):
        return lax.rem(r + d, nrow)

    barrier = pltpu.get_barrier_semaphore()
    for d in range(1, nrow):
        pl.semaphore_signal(barrier, inc=1, device_id={"row": row_at(d)}, device_id_type=MESH)
    pl.semaphore_wait(barrier, nrow - 1)

    def scatter(d):
        return pltpu.make_async_remote_copy(
            p_ref.at[row_at(d)], recv.at[d], send_sem.at[d], recv_sem.at[d],
            device_id={"row": row_at(d)}, device_id_type=MESH)

    for d in range(1, nrow):
        scatter(d).start()
    total = p_ref[r]
    for d in range(1, nrow):
        scatter(d).wait_recv()
        total = total + recv[d]
    out_ref[...] = total
    for d in range(1, nrow):
        scatter(d).wait_send()


def sum_scatter(p, nrow):
    chunk = (p.shape[0] // nrow, p.shape[1])
    sem = pltpu.SemaphoreType.DMA
    return pl.pallas_call(
        functools.partial(sum_scatter_kernel, nrow),
        out_shape=jax.ShapeDtypeStruct(chunk, jnp.float32),
        in_specs=[pl.BlockSpec(memory_space=pltpu.VMEM)],
        out_specs=pl.BlockSpec(memory_space=pltpu.VMEM),
        scratch_shapes=[pltpu.VMEM((nrow,) + chunk, jnp.float32), sem((nrow,)), sem((nrow,))],
        compiler_params=pltpu.CompilerParams(collective_id=1, has_side_effects=True),
        cost_estimate=pl.CostEstimate(flops=0, bytes_accessed=30_000_000, transcendentals=0),
        name="sum_scatter",
    )(p.reshape((nrow,) + chunk))


def on_device(nrow, ncol, eigvecs, reflectors, factors, slab):
    c = lax.axis_index("col")
    even = lax.rem(c, 2) == 0
    pairs = ncol // 2
    own = reflectors.shape[2]
    near = pairs <= 2
    swap = [(i, i + 1 - 2 * (i % 2)) for i in range(ncol)]

    def cross(block):
        return [block] + [
            lax.ppermute(block, "col", [(i, (i + 2 * s) % ncol) for i in range(ncol)]) for s in range(1, pairs)
        ]

    def pair_up(blocks):
        mates = [lax.ppermute(block, "col", swap) for block in blocks]
        return [
            jnp.concatenate([jnp.where(even, a, b), jnp.where(even, b, a)], axis=1) for a, b in zip(blocks, mates)
        ]

    def reorder(stacked, axis):
        if not near or pairs == 1:
            return stacked
        turned = jnp.roll(stacked, stacked.shape[axis] // 2, axis)
        return jnp.where(c // 2 == 0, stacked, turned)

    first_own, second_own = reflectors[0], reflectors[1]
    if near:
        crossed_x = cross(eigvecs)
        crossed_second = cross(second_own)
        late_own, *crossed_x = lax.optimization_barrier((first_own, *crossed_x))
        crossed_first = cross(late_own)
        all_x, second_y, first_y = pair_up(crossed_x), pair_up(crossed_second), pair_up(crossed_first)
    else:
        all_x, second_y, first_y = (
            [lax.all_gather(block, "col", axis=1, tiled=True)] for block in (eigvecs, second_own, first_own)
        )

    both = jnp.concatenate([second_own, first_own], axis=1)
    by_x = jnp.concatenate([tdot(both, x) for x in all_x], axis=1)
    by_y = jnp.concatenate([tdot(first_own, y) for y in second_y], axis=1)
    stacked = reorder(jnp.concatenate([by_x, by_y]), 1)

    def by_slab(blocks):
        return [dot(y, slab, ((0,), (1,))) for y in blocks]

    slab_x, slab_second, slab_first = by_slab(all_x), by_slab(second_y), by_slab(first_y[:1])
    if near:
        stacked, slab_x, slab_second[:1], slab_first = lax.optimization_barrier(
            (stacked, slab_x, slab_second[:1], slab_first)
        )
        sums = sum_gather(stacked, nrow, ncol)
    else:
        sums = lax.all_gather(lax.psum(stacked, "row"), "col")
    if near and pairs > 1:
        late, sums = lax.optimization_barrier((first_y[1:], sums))
        first_y = first_y[:1] + list(late)
    slab_first = slab_first + by_slab(first_y[1:])

    panel = factors.shape[1]
    second_w, first_raw, gram = (
        sums[:, i * own : (i + 1) * own].reshape(panel, -1) for i in range(3)
    )
    second_tw = dot(factors[1], second_w)
    first_tw = dot(factors[0], first_raw - dot(gram, second_tw))
    second_tw, first_tw = reorder(second_tw, 0), reorder(first_tw, 0)
    partial = (
        reorder(jnp.concatenate(slab_x), 0)
        - tdot(second_tw, jnp.concatenate(slab_second))
        - tdot(first_tw, jnp.concatenate(slab_first))
    )
    product = sum_scatter(partial, nrow)

    vectors = eigvecs
    width = panel // len(first_y)
    for blocks, tw in ((second_y, second_tw), (first_y, first_tw)):
        mine = lax.dynamic_slice_in_dim(tw, c * eigvecs.shape[1], eigvecs.shape[1], axis=1)
        for s, y in enumerate(blocks):
            vectors = vectors - dot(y, mine[s * width : (s + 1) * width])
    return vectors, product.T


def solution(mesh):
    return jax.shard_map(
        functools.partial(on_device, mesh.shape["row"], mesh.shape["col"]),
        mesh=mesh,
        in_specs=(P("row", "col"), P(None, "row", "col"), P(), P("col", "row")),
        out_specs=(P("row", "col"), P("col", "row")),
        check_vma=False,
    )
```

```python
import functools

import jax
import jax.numpy as jnp
from jax import lax
from jax.experimental import pallas as pl
from jax.experimental.pallas import tpu as pltpu
from jax.sharding import PartitionSpec as P


MESH = pl.DeviceIdType.MESH


def dot(left, right, dims=((1,), (0,))):
    return lax.dot_general(
        left, right, (dims, ((), ())), precision=lax.Precision.HIGH, preferred_element_type=jnp.float32
    )


def tdot(left, right):
    return dot(left, right, ((0,), (0,)))


def sum_gather_kernel(nrow, ncol, m_ref, out_ref, recv, rs_send, rs_recv, a_send, a_recv, x_send, x_recv, c_send, c_recv):
    r, c = lax.axis_index("row"), lax.axis_index("col")
    pairs = ncol // 2
    mate = c + 1 - 2 * lax.rem(c, 2)

    def row_at(d):
        return lax.rem(r + d + nrow, nrow)

    def col_at(s):
        return lax.rem(c + 2 * s + ncol, ncol)

    barrier = pltpu.get_barrier_semaphore()
    for d in range(1, nrow):
        pl.semaphore_signal(barrier, inc=1, device_id=(row_at(d), c), device_id_type=MESH)
    for s in range(1, pairs):
        pl.semaphore_signal(barrier, inc=1, device_id=(r, col_at(s)), device_id_type=MESH)
    pl.semaphore_signal(barrier, inc=1, device_id=(r, mate), device_id_type=MESH)
    pl.semaphore_wait(barrier, nrow - 1 + pairs - 1 + 1)

    def scatter(d):
        return pltpu.make_async_remote_copy(
            m_ref.at[row_at(d)], recv.at[d], rs_send.at[d], rs_recv.at[d],
            device_id=(row_at(d), c), device_id_type=MESH)

    for d in range(1, nrow):
        scatter(d).start()
    total = m_ref[r]
    for d in range(1, nrow):
        scatter(d).wait_recv()
        total = total + recv[d]
    out_ref[c, r] = total

    def along_row(d):
        return pltpu.make_async_remote_copy(
            out_ref.at[c, r], out_ref.at[c, r], a_send.at[d], a_recv.at[d],
            device_id=(row_at(d), c), device_id_type=MESH)

    def across(s, d):
        chunk = out_ref.at[c, row_at(-d)]
        return pltpu.make_async_remote_copy(
            chunk, chunk, x_send.at[s, d], x_recv.at[s, d],
            device_id=(r, col_at(s)), device_id_type=MESH)

    def to_mate(s, d):
        chunk = out_ref.at[col_at(-s), row_at(-d)]
        return pltpu.make_async_remote_copy(
            chunk, chunk, c_send.at[s, d], c_recv.at[s, d],
            device_id=(r, mate), device_id_type=MESH)

    for s in range(1, pairs):
        across(s, 0).start()
    for d in range(1, nrow):
        along_row(d).start()
    to_mate(0, 0).start()
    for d in range(1, nrow):
        along_row(d).wait_recv()
        for s in range(1, pairs):
            across(s, d).start()
        to_mate(0, d).start()
    for d in range(nrow):
        for s in range(1, pairs):
            across(s, d).wait_recv()
            to_mate(s, d).start()
    for d in range(nrow):
        for s in range(pairs):
            to_mate(s, d).wait_recv()
    for d in range(1, nrow):
        scatter(d).wait_send()
        along_row(d).wait_send()
    for d in range(nrow):
        for s in range(pairs):
            to_mate(s, d).wait_send()
            if s:
                across(s, d).wait_send()


def sum_gather(m, nrow, ncol):
    chunk = (m.shape[0] // nrow, m.shape[1])
    pairs = ncol // 2
    sem = pltpu.SemaphoreType.DMA
    out = pl.pallas_call(
        functools.partial(sum_gather_kernel, nrow, ncol),
        out_shape=jax.ShapeDtypeStruct((ncol, nrow) + chunk, jnp.float32),
        in_specs=[pl.BlockSpec(memory_space=pltpu.VMEM)],
        out_specs=pl.BlockSpec(memory_space=pltpu.VMEM),
        scratch_shapes=[
            pltpu.VMEM((nrow,) + chunk, jnp.float32),
            sem((nrow,)), sem((nrow,)), sem((nrow,)), sem((nrow,)),
            sem((pairs, nrow)), sem((pairs, nrow)), sem((pairs, nrow)), sem((pairs, nrow)),
        ],
        compiler_params=pltpu.CompilerParams(collective_id=0, has_side_effects=True),
        cost_estimate=pl.CostEstimate(flops=0, bytes_accessed=60_000_000, transcendentals=0),
        name="sum_gather",
    )(m.reshape((nrow,) + chunk))
    return out.reshape((ncol,) + m.shape)


def sum_scatter_kernel(nrow, p_ref, out_ref, recv, send_sem, recv_sem):
    r = lax.axis_index("row")

    def row_at(d):
        return lax.rem(r + d, nrow)

    barrier = pltpu.get_barrier_semaphore()
    for d in range(1, nrow):
        pl.semaphore_signal(barrier, inc=1, device_id={"row": row_at(d)}, device_id_type=MESH)
    pl.semaphore_wait(barrier, nrow - 1)

    def scatter(d):
        return pltpu.make_async_remote_copy(
            p_ref.at[row_at(d)], recv.at[d], send_sem.at[d], recv_sem.at[d],
            device_id={"row": row_at(d)}, device_id_type=MESH)

    for d in range(1, nrow):
        scatter(d).start()
    total = p_ref[r]
    for d in range(1, nrow):
        scatter(d).wait_recv()
        total = total + recv[d]
    out_ref[...] = total
    for d in range(1, nrow):
        scatter(d).wait_send()


def sum_scatter(p, nrow):
    chunk = (p.shape[0] // nrow, p.shape[1])
    sem = pltpu.SemaphoreType.DMA
    return pl.pallas_call(
        functools.partial(sum_scatter_kernel, nrow),
        out_shape=jax.ShapeDtypeStruct(chunk, jnp.float32),
        in_specs=[pl.BlockSpec(memory_space=pltpu.VMEM)],
        out_specs=pl.BlockSpec(memory_space=pltpu.VMEM),
        scratch_shapes=[pltpu.VMEM((nrow,) + chunk, jnp.float32), sem((nrow,)), sem((nrow,))],
        compiler_params=pltpu.CompilerParams(collective_id=1, has_side_effects=True),
        cost_estimate=pl.CostEstimate(flops=0, bytes_accessed=30_000_000, transcendentals=0),
        name="sum_scatter",
    )(p.reshape((nrow,) + chunk))


def on_device(nrow, ncol, eigvecs, reflectors, factors, slab):
    c = lax.axis_index("col")
    even = lax.rem(c, 2) == 0
    pairs = ncol // 2
    own = reflectors.shape[2]
    near = pairs <= 2
    swap = [(i, i + 1 - 2 * (i % 2)) for i in range(ncol)]

    def cross(block):
        return [block] + [
            lax.ppermute(block, "col", [(i, (i + 2 * s) % ncol) for i in range(ncol)]) for s in range(1, pairs)
        ]

    def pair_up(blocks):
        mates = [lax.ppermute(block, "col", swap) for block in blocks]
        return [
            jnp.concatenate([jnp.where(even, a, b), jnp.where(even, b, a)], axis=1) for a, b in zip(blocks, mates)
        ]

    def reorder(stacked, axis):
        if not near or pairs == 1:
            return stacked
        turned = jnp.roll(stacked, stacked.shape[axis] // 2, axis)
        return jnp.where(c // 2 == 0, stacked, turned)

    first_own, second_own = reflectors[0], reflectors[1]
    if near:
        crossed_x = cross(eigvecs)
        crossed_second = cross(second_own)
        late_own, *crossed_x = lax.optimization_barrier((first_own, *crossed_x))
        crossed_first = cross(late_own)
        all_x, second_y, first_y = pair_up(crossed_x), pair_up(crossed_second), pair_up(crossed_first)
    else:
        all_x, second_y, first_y = (
            [lax.all_gather(block, "col", axis=1, tiled=True)] for block in (eigvecs, second_own, first_own)
        )

    both = jnp.concatenate([second_own, first_own], axis=1)
    by_x = []
    for x in all_x:
        by_x.append(tdot(both, x))
    by_x = jnp.concatenate(by_x, axis=1)
    by_y = jnp.concatenate([tdot(first_own, y) for y in second_y], axis=1)
    stacked = reorder(jnp.concatenate([by_x, by_y]), 1)

    def by_slab(blocks):
        out = []
        for y in blocks:
            out.append(dot(y, slab, ((0,), (1,))))
        return out

    slab_x, slab_second, slab_first = (by_slab(all_x), by_slab(second_y[:1]), by_slab(first_y[:1]))
    if near:
        stacked, slab_x, slab_second, slab_first = lax.optimization_barrier(
            (stacked, slab_x, slab_second, slab_first)
        )
        sums = sum_gather(stacked, nrow, ncol)
    else:
        sums = lax.all_gather(lax.psum(stacked, "row"), "col")
    if near and pairs > 1:
        late, second_y[1], sums = lax.optimization_barrier((first_y[1:], second_y[1], sums))
        first_y = first_y[:1] + list(late)
    slab_second = slab_second + by_slab(second_y[1:])
    slab_first = slab_first + by_slab(first_y[1:])

    panel = factors.shape[1]
    second_w, first_raw, gram = (
        sums[:, i * own : (i + 1) * own].reshape(panel, -1) for i in range(3)
    )
    second_tw = dot(factors[1], second_w)
    first_tw = dot(factors[0], first_raw - dot(gram, second_tw))
    second_tw, first_tw = reorder(second_tw, 0), reorder(first_tw, 0)
    partial = (
        reorder(jnp.concatenate(slab_x), 0)
        - tdot(second_tw, jnp.concatenate(slab_second))
        - tdot(first_tw, jnp.concatenate(slab_first))
    )
    product = sum_scatter(partial, nrow)

    vectors = eigvecs
    width = panel // len(first_y)
    for blocks, tw in ((second_y, second_tw), (first_y, first_tw)):
        mine = lax.dynamic_slice_in_dim(tw, c * eigvecs.shape[1], eigvecs.shape[1], axis=1)
        for s, y in enumerate(blocks):
            vectors = vectors - dot(y, mine[s * width : (s + 1) * width])
    return vectors, product.T


def solution(mesh):
    nrow, ncol = mesh.shape["row"], mesh.shape["col"]
    return jax.shard_map(
        functools.partial(on_device, nrow, ncol),
        mesh=mesh,
        in_specs=(P("row", "col"), P(None, "row", "col"), P(), P("col", "row")),
        out_specs=(P("row", "col"), P("col", "row")),
        check_vma=False,
    )
```
